1024 devices in a mesh: gx: 64 (over x_hi, z, core), gy: 16 (over y, x_lo).
Axes of the slice: x: 4 (x_hi: 2, x_lo: 2; x = x_hi * 2 + x_lo), y: 8, z: 16, core: 2. Of those that a mesh axis runs over, the one named last changes fastest.
Arguments:
- density: float32 [1024, 768, 128], P('gx', 'gy'), may hold values from -6 to 6
- momenta: float32 [3, 1024, 768, 128], P(None, 'gx', 'gy'), may hold values from -6 to 6
- smooth_taps: float32 [33], replicated, may hold values from -1 to 1
- deriv_taps: float32 [33], replicated, may hold values from -1 to 1
- kick_step: float32 [], replicated, may hold values from 0.5 to 1.5
Outputs:
- kicked: float32 [3, 1024, 768, 128], P(None, 'gx', 'gy')
The draws below stay inside these ranges and needn't reach their ends.
All inputs are finite; a program needn't handle non-finite values.
Results may differ from the reference program's by a relative error of at most 0.00007.
Values sent between devices are 32-bit elements; how exact they have to be, the bound alone decides.
A program may use at most 64 MiB of HBM per device.

```python
import jax
import jax.numpy as jnp
from jax import lax

NZ = 128
RADIUS = 16
FACTOR = 4
NX = 1024
NY = 768
CNX = 256
CNY = 192
CNZ = 32


def level_of(key, extent, split, smallest, high):
    gain, own = 1.0, jax.random.fold_in(key, 6)
    for dim, blocks in split:
        steps = jnp.exp(jax.random.uniform(jax.random.fold_in(own, dim), (blocks,), jnp.float32, smallest / len(split), high / len(split)))
        gain = gain * jnp.repeat(steps, extent[dim] // blocks).reshape([-1 if axis == dim else 1 for axis in range(len(extent))])
    return gain


def noise(stream_key, extent, scale, most, shards=(), held_as=jnp.bfloat16):
    drawn = jax.random.normal(stream_key, extent, jnp.float32) * scale
    if len(shards) > 0:
        drawn = level_of(stream_key, extent, shards, -0.22, 0.18) * drawn
    return jnp.clip(drawn, min=-most, max=most).astype(held_as)


def setup_inputs(seed: int = 0) -> dict:
    seeds = jax.random.split(jax.random.key(seed), 6)
    density = noise(seeds[0], (NX, NY, NZ), 1.0, 6.0, ((0, 64), (1, 16)), jnp.float32)
    momenta = noise(seeds[1], (3, NX, NY, NZ), 1.0, 6.0, ((1, 64), (2, 16)), jnp.float32)
    smooth_taps = noise(seeds[2], (2 * RADIUS + 1,), (2 * RADIUS + 1) ** -0.5, 1.0, (), jnp.float32)
    deriv_taps = noise(seeds[3], (2 * RADIUS + 1,), (2 * RADIUS + 1) ** -0.5, 1.0, (), jnp.float32)
    kick_step = jnp.clip(jax.random.uniform(seeds[4], (), jnp.float32, 0.5, 1.5), 0.5, 1.5)
    return {"density": density, "momenta": momenta, "smooth_taps": smooth_taps, "deriv_taps": deriv_taps, "kick_step": kick_step}


LONG_COUPLING = 16.0


def convolve(field, weights, along):
    def add_tap(tap_step, total):
        return total + weights[tap_step] * jnp.roll(field, RADIUS - tap_step, along)
    return lax.fori_loop(0, 2 * RADIUS + 1, add_tap, jnp.zeros_like(field))


def long_forces(density):
    coarse = density.reshape(CNX, FACTOR, CNY, FACTOR, CNZ, FACTOR).mean(axis=(1, 3, 5))
    spectrum = jnp.fft.fftn(coarse)
    phase_x = 2.0 * jnp.pi * jnp.arange(CNX) / CNX
    phase_y = 2.0 * jnp.pi * jnp.arange(CNY) / CNY
    phase_z = 2.0 * jnp.pi * jnp.arange(CNZ) / CNZ
    laplace = (2.0 - 2.0 * jnp.cos(phase_x))[:, None, None] + (2.0 - 2.0 * jnp.cos(phase_y))[None, :, None] + (2.0 - 2.0 * jnp.cos(phase_z))[None, None, :]
    anchor = laplace.shape[0] * 0
    safe = laplace.at[anchor, anchor, anchor].set(1.0)
    inverse = (1.0 / safe).at[anchor, anchor, anchor].set(0.0)
    sine_list = [jnp.sin(phase_x)[:, None, None], jnp.sin(phase_y)[None, :, None], jnp.sin(phase_z)[None, None, :]]
    return [jnp.real(jnp.fft.ifftn(1j * sine_part * spectrum * inverse)) for sine_part in sine_list]


def reference(density, momenta, smooth_taps, deriv_taps, kick_step):
    smooth_x = convolve(density, smooth_taps, 0)
    deriv_x = convolve(density, deriv_taps, 0)
    smooth_xy = convolve(smooth_x, smooth_taps, 1)
    short_range = [convolve(convolve(deriv_x, smooth_taps, 1), smooth_taps, 2),
                   convolve(convolve(smooth_x, deriv_taps, 1), smooth_taps, 2),
                   convolve(smooth_xy, deriv_taps, 2)]
    long_range = long_forces(density)
    kicked = []
    for component in range(3):
        fine_long = jnp.repeat(jnp.repeat(jnp.repeat(long_range[component], FACTOR, 0), FACTOR, 1), FACTOR, 2)
        kicked.append(momenta[component] + kick_step * (short_range[component] + LONG_COUPLING * fine_long))
    return jnp.stack(kicked)
```

```python
import functools
import math

import jax
import jax.numpy as jnp
import numpy as np
from jax import lax
from jax.experimental import pallas as pl
from jax.experimental.pallas import tpu as pltpu
from jax.sharding import PartitionSpec as P

FACTOR = 4
RADIUS = 16
LONG_COUPLING = 16.0
HIGHEST = lax.Precision.HIGHEST
MESH = pl.DeviceIdType.MESH
F32 = jnp.float32

T_P, T_Q, T_A, T_B, T_C, T_G, T_W, T_ROWS = 0, 16, 32, 64, 96, 128, 176, 184
C_ZF, C_ZI, C_ZD, C_YF, C_YI, C_ROWS = 0, 32, 64, 96, 608, 1120


def z_basis():
    n = np.arange(32)
    basis = np.zeros((2, 16, 32))
    norm = np.full((2, 16), 2.0 / 32)
    for g in range(16):
        basis[0, g] = np.cos(2 * np.pi * g * n / 32)
        basis[1, g] = np.sin(2 * np.pi * g * n / 32)
    basis[1, 0] = np.cos(np.pi * n)
    norm[:, 0] = 1.0 / 32
    return basis.reshape(32, 32), norm.reshape(32)


def y_basis(count):
    half = count // 2
    wave = np.array([m if m <= half else m - half for m in range(count)])
    y = np.arange(count)
    angle = 2 * np.pi / count * (wave[:, None] * y[None, :] % count)
    is_cos = (np.arange(count) <= half)[:, None]
    basis = np.where(is_cos, np.cos(angle), np.sin(angle))
    norm = np.where((wave == 0) | (wave == half), 1.0, 2.0) / count
    return basis, norm, wave


def shared_constants():
    out = np.zeros((C_ROWS, 128))
    zb, zn = z_basis()
    out[C_ZF : C_ZF + 32] = np.repeat(zb, 4, axis=1) / 64.0
    zi = zb * zn[:, None] * LONG_COUPLING
    out[C_ZI : C_ZI + 32] = np.repeat(zi, 4, axis=1)
    zd = 0.5 * (np.roll(zi, -1, axis=1) - np.roll(zi, 1, axis=1))
    out[C_ZD : C_ZD + 32] = np.repeat(zd, 4, axis=1)
    yb, yn, _ = y_basis(192)
    for tile in range(2):
        for half in range(2):
            fwd = np.zeros((128, 128))
            inv = np.zeros((128, 128))
            fwd[:96, :96] = yb[96 * half : 96 * half + 96, 96 * tile : 96 * tile + 96].T
            for jj in range(8):
                for p in range(14):
                    y = (12 * (8 * tile + jj) - 1 + p) % 192
                    cols = slice(96 * half, 96 * half + 96)
                    inv[:96, 16 * jj + p] = yb[cols, y] * yn[cols]
            row = C_YF + (2 * tile + half) * 128
            out[row : row + 128] = fwd
            row = C_YI + (2 * half + tile) * 128
            out[row : row + 128] = inv
    return out.astype(np.float32)


def solve_tables(chips):
    n = 8 * chips
    out = np.zeros((16, 2, T_ROWS, 128))
    _, _, wave = y_basis(192)
    for g in range(16):
        for half in range(2):
            t = out[g, half]
            ky = wave[96 * half : 96 * half + 96]
            for c in range(2):
                kz = 16 if (g == 0 and c == 1) else g
                a = np.ones(128)
                a[:96] = (2 - 2 * np.cos(2 * np.pi * ky / 192)) + (2 - 2 * np.cos(2 * np.pi * kz / 32))
                zero = np.zeros(128, bool)
                zero[:96] = (ky == 0) & (kz == 0)
                a[zero] = 1.0
                r = 1 + a / 2 - np.sqrt(a + a * a / 4)
                den = (1 / r - r) * (1 - r**n)
                pick = lambda general, special: np.where(zero, special, general)
                for sc in range(2):
                    for xl in range(4):
                        x8 = 4 * sc + xl
                        t[T_P + sc * 8 + c * 4 + xl] = pick(r ** (-x8), 1.0)
                        t[T_Q + sc * 8 + c * 4 + xl] = pick(r**x8, float(x8))
                for ct in range(2):
                    for i in range(6):
                        x8 = 4 * ct - 1 + i
                        row = ct * 16 + c * 8 + i
                        t[T_A + row] = pick(r ** float(x8) / den, -x8 / 2 + x8 * x8 / (2 * n))
                        t[T_B + row] = pick(r ** float(-x8) / den, -x8 / n)
                        t[T_C + row] = pick(0.0, 8 * x8 / n)
                for o in range(17):
                    d = abs(o - 8)
                    t[T_G + c * 24 + o] = pick((r**d + r ** (n - d)) / den, -d * (n - d) / (2 * n))
                for pq in range(2):
                    t[T_W + pq * 2 + c] = pick(r**8, 1.0)
    return out.reshape(32, T_ROWS, 128).astype(np.float32)


def dot(a, b):
    return lax.dot_general(a, b, (((1,), (0,)), ((), ())), precision=HIGHEST, preferred_element_type=F32)


def dot_nt(a, b):
    return lax.dot_general(a, b, (((1,), (1,)), ((), ())), precision=HIGHEST, preferred_element_type=F32)


def wrap(value, count):
    return lax.rem(value + count, count)


def send_order(chips):
    ring = min(16, chips)
    def hops(step):
        along = step % ring
        return min(along, ring - along) + (2 if step >= ring else 0)
    return sorted(range(1, chips), key=lambda step: (-hops(step), step))


def kernel(
    gx_count, density, cst_hbm, tab_hbm, padded, long_ref,
    cst, tab, m1, r1, fs, pair, mom, r2, os_, pair2, ps, r3,
    load_sem, strip_send, strip_recv, tile_send, tile_recv, corner_send, corner_recv,
    m_send, m_recv, p_send, p_recv,
):
    gx = lax.axis_index("gx")
    gy = lax.axis_index("gy")
    chips = gx_count // 2
    core = lax.rem(gx, 2)
    chip = gx // 2
    partner = gx + 1 - 2 * core
    outer = wrap(gx + 2 * core - 1, gx_count)

    barrier = pltpu.get_barrier_semaphore()

    def greet(device):
        pl.semaphore_signal(barrier, inc=1, device_id=device, device_id_type=MESH)

    for step in send_order(chips):
        greet({"gx": 2 * lax.rem(chip + step, chips) + core})
    for step in range(1, 16):
        greet({"gy": lax.rem(gy + step, 16)})
    greet({"gx": outer})
    greet({"gx": partner})

    loads = [
        pltpu.make_async_copy(density, padded.at[16:32, 16:64], load_sem.at[0]),
        pltpu.make_async_copy(cst_hbm, cst, load_sem.at[1]),
        pltpu.make_async_copy(tab_hbm.at[2 * gy + core], tab, load_sem.at[2]),
    ]
    for load in loads:
        load.start()
    for load in loads:
        load.wait()

    lane = lax.broadcasted_iota(jnp.int32, (48, 128), 1)
    block = lax.broadcasted_iota(jnp.int32, (48, 128), 0) // 4
    placed = (lane == block + 12 * lax.rem(gy, 8)).astype(F32)
    zf = cst[C_ZF : C_ZF + 32]
    for xl in range(4):
        rows = padded[16 + 4 * xl, 16:64]
        for fine in range(1, 4):
            rows = rows + padded[16 + 4 * xl + fine, 16:64]
        spread = dot(dot_nt(zf, rows), placed)
        for c in range(2):
            m1[:, c * 4 + xl, :] = spread[16 * c : 16 * c + 16]

    pl.semaphore_wait(barrier, (chips - 1) + 15 + 2)

    def remote(src, dst, send_sem, recv_sem, device):
        return pltpu.make_async_remote_copy(
            src_ref=src, dst_ref=dst, send_sem=send_sem, recv_sem=recv_sem,
            device_id=device, device_id_type=MESH,
        )

    for step in (8, 7, 9, 6, 10, 5, 11, 4, 12, 3, 13, 2, 14, 1, 15):
        target = lax.rem(gy + step, 16)
        remote(m1.at[target], r1.at[gy], m_send.at[0], m_recv.at[0], {"gy": target}).start()
    below, above = wrap(gy - 1, 16), lax.rem(gy + 1, 16)
    strips = [
        remote(padded.at[16:32, 16:32], padded.at[16:32, 64:80], strip_send.at[0], strip_recv.at[0], {"gy": below}),
        remote(padded.at[16:32, 48:64], padded.at[16:32, 0:16], strip_send.at[1], strip_recv.at[1], {"gy": above}),
    ]
    back, ahead = wrap(gx - 1, gx_count), lax.rem(gx + 1, gx_count)
    tiles = [
        remote(padded.at[16:32, 16:64], padded.at[32:48, 16:64], tile_send.at[0], tile_recv.at[0], {"gx": back}),
        remote(padded.at[16:32, 16:64], padded.at[0:16, 16:64], tile_send.at[1], tile_recv.at[1], {"gx": ahead}),
    ]
    for copy in strips + tiles:
        copy.start()

    r1[gy] = m1[gy]
    pltpu.make_async_copy(r1.at[0:15], r1.at[0:15], m_recv.at[0]).wait()
    low = r1[0]
    high = r1[8]
    for j in range(1, 8):
        low = low + r1[j]
        high = high + r1[8 + j]
    for half in range(2):
        first = C_YF + half * 128
        second = C_YF + (2 + half) * 128
        fs[half] = dot(low, cst[first : first + 128]) + dot(high, cst[second : second + 128])
    swap = remote(fs.at[1 - core], pair.at[core], p_send.at[0], p_recv.at[0], {"gx": partner})
    swap.start()
    pair[core] = fs[core]
    swap.wait_recv()

    e0 = pair[0]
    e1 = pair[1]
    for pq, table in ((0, T_P), (1, T_Q)):
        terms = e0 * tab[table : table + 8] + e1 * tab[table + 8 : table + 16]
        for c in range(2):
            mom[2 * pq + c : 2 * pq + c + 1, :] = jnp.sum(terms[4 * c : 4 * c + 4], axis=0, keepdims=True)
    for step in send_order(chips):
        target = 2 * lax.rem(chip + step, chips) + core
        remote(mom, r2.at[step], m_send.at[1], m_recv.at[1], {"gx": target}).start()

    for copy in strips:
        copy.wait_recv()
    corners = []
    for side, cols in enumerate((slice(0, 16), slice(64, 80))):
        corners.append(remote(padded.at[16:32, cols], padded.at[32:48, cols], corner_send.at[2 * side], corner_recv.at[2 * side], {"gx": back}))
        corners.append(remote(padded.at[16:32, cols], padded.at[0:16, cols], corner_send.at[2 * side + 1], corner_recv.at[2 * side + 1], {"gx": ahead}))
    for copy in corners:
        copy.start()

    pltpu.make_async_copy(r2.at[1:chips], r2.at[1:chips], m_recv.at[1]).wait()
    ratio = tab[T_W : T_W + 4]
    is_first = lax.broadcasted_iota(jnp.int32, (4, 128), 0) < 2
    total = jnp.zeros((4, 128), F32)
    ramp = jnp.zeros((4, 128), F32)
    for step in range(chips - 1, 0, -1):
        total = (total + jnp.where(is_first, r2[step], r2[chips - step])) * ratio
        ramp = ramp + total
    for ct in range(2):
        for c in range(2):
            row = ct * 16 + c * 8
            phi = (
                tab[T_A + row : T_A + row + 8] * total[c : c + 1]
                + tab[T_B + row : T_B + row + 8] * total[2 + c : 3 + c]
                + tab[T_C + row : T_C + row + 8] * ramp[c : c + 1]
            )
            for x8 in range(8):
                source = (e0 if x8 < 4 else e1)[c * 4 + x8 % 4 : c * 4 + x8 % 4 + 1]
                start = T_G + c * 24 + 7 + 4 * ct - x8
                phi = phi + tab[start : start + 8] * source
            os_[ct, c * 8 : c * 8 + 8, :] = phi
    swap2 = remote(os_.at[1 - core], pair2.at[core], p_send.at[1], p_recv.at[1], {"gx": partner})
    swap2.start()
    pair2[core] = os_[core]
    swap2.wait_recv()

    h0 = pair2[0]
    h1 = pair2[1]
    for tile in range(2):
        first = C_YI + tile * 128
        second = C_YI + (2 + tile) * 128
        ps[tile] = dot(h0, cst[first : first + 128]) + dot(h1, cst[second : second + 128])
    for step in (8, 7, 9, 6, 10, 5, 11, 4, 12, 3, 13, 2, 14, 1, 15):
        target = lax.rem(gy + step, 16)
        remote(ps.at[target // 8], r3.at[gy], m_send.at[2], m_recv.at[2], {"gy": target}).start()
    r3[gy] = ps[gy // 8]

    for copy in tiles + corners:
        copy.wait_recv()

    pltpu.make_async_copy(r3.at[0:15], r3.at[0:15], m_recv.at[2]).wait()
    here = block + 16 * lax.rem(gy, 8) + 1
    at_cell = (lane == here).astype(F32)
    slope = 0.5 * (lane == here + 1).astype(F32) - 0.5 * (lane == here - 1).astype(F32)
    along = []
    across = []
    for i in range(6):
        coeffs = jnp.concatenate([r3[:, i, :], r3[:, 8 + i, :]], axis=0)
        along.append(dot_nt(at_cell, coeffs))
        if 1 <= i <= 4:
            across.append(dot_nt(slope, coeffs))
    zi = cst[C_ZI : C_ZI + 32]
    zd = cst[C_ZD : C_ZD + 32]
    for xl in range(4):
        long_ref[0, xl] = dot(0.5 * (along[xl + 2] - along[xl]), zi)
        long_ref[1, xl] = dot(across[xl], zi)
        long_ref[2, xl] = dot(along[xl + 1], zd)

    for copy in strips + tiles + corners + [swap, swap2]:
        copy.wait_send()
    pltpu.make_async_copy(m1.at[0:15], m1.at[0:15], m_send.at[0]).wait()
    pltpu.make_async_copy(r2.at[1:chips], r2.at[1:chips], m_send.at[1]).wait()
    pltpu.make_async_copy(r3.at[0:15], r3.at[0:15], m_send.at[2]).wait()


def exchange(density, gx_count):
    chips = gx_count // 2
    any_spec = pl.BlockSpec(memory_space=pl.ANY)
    vmem_spec = pl.BlockSpec(memory_space=pltpu.VMEM)
    vm = lambda *shape: pltpu.VMEM(shape, F32)
    dma = lambda n: pltpu.SemaphoreType.DMA((n,))
    return pl.pallas_call(
        functools.partial(kernel, gx_count),
        out_shape=(
            jax.ShapeDtypeStruct((48, 80, 128), F32),
            jax.ShapeDtypeStruct((3, 4, 48, 128), F32),
        ),
        in_specs=[any_spec] * 3,
        out_specs=(vmem_spec, vmem_spec),
        scratch_shapes=[
            vm(C_ROWS, 128), vm(T_ROWS, 128), vm(16, 8, 128), vm(16, 8, 128), vm(2, 8, 128), vm(2, 8, 128),
            vm(4, 128), vm(chips, 4, 128), vm(2, 16, 128), vm(2, 16, 128), vm(2, 16, 128), vm(16, 16, 128),
            dma(3), dma(2), dma(2), dma(2), dma(2), dma(4), dma(4), dma(3), dma(3), dma(2), dma(2),
        ],
        compiler_params=pltpu.CompilerParams(collective_id=0, has_side_effects=True),
    )(density, jnp.asarray(shared_constants()), jnp.asarray(solve_tables(chips)))


def band_matrix(weights, sources, targets, shift, period):
    source_idx = lax.broadcasted_iota(jnp.int32, (sources, targets), 0)
    target_idx = lax.broadcasted_iota(jnp.int32, (sources, targets), 1)
    offset = source_idx - target_idx + shift
    if period > 0:
        offset = offset % period
    tap_index = jnp.arange(weights.shape[0], dtype=jnp.int32)
    one_hot = (offset[:, :, None] == tap_index[None, None, :]).astype(jnp.float32)
    return jnp.einsum("abt,t->ab", one_hot, weights, precision=HIGHEST)


def short_forces(padded, smooth_taps, deriv_taps):
    smooth_rows = band_matrix(smooth_taps, 48, 16, 0, 0)
    deriv_rows = band_matrix(deriv_taps, 48, 16, 0, 0)
    smooth_x = jnp.einsum("jyz,ji->iyz", padded, smooth_rows, precision=HIGHEST)
    deriv_x = jnp.einsum("jyz,ji->iyz", padded, deriv_rows, precision=HIGHEST)
    smooth_cols = band_matrix(smooth_taps, 80, 48, 0, 0)
    deriv_cols = band_matrix(deriv_taps, 80, 48, 0, 0)
    smooth_depth = band_matrix(smooth_taps, 128, 128, RADIUS, 128)
    deriv_depth = band_matrix(deriv_taps, 128, 128, RADIUS, 128)
    first = jnp.einsum("xjz,ji->xiz", deriv_x, smooth_cols, precision=HIGHEST)
    second = jnp.einsum("xjz,ji->xiz", smooth_x, deriv_cols, precision=HIGHEST)
    third = jnp.einsum("xjz,ji->xiz", smooth_x, smooth_cols, precision=HIGHEST)
    return jnp.stack(
        [
            jnp.einsum("xyj,ji->xyi", first, smooth_depth, precision=HIGHEST),
            jnp.einsum("xyj,ji->xyi", second, smooth_depth, precision=HIGHEST),
            jnp.einsum("xyj,ji->xyi", third, deriv_depth, precision=HIGHEST),
        ]
    )


def per_device(density, momenta, smooth_taps, deriv_taps, kick_step):
    padded, long_range = exchange(density, lax.axis_size("gx"))
    short_range = short_forces(padded, smooth_taps, deriv_taps)
    long_rows = jnp.broadcast_to(long_range[:, :, None], (3, 4, FACTOR, 48, 128)).reshape(3, 16, 48, 128)
    return momenta + kick_step * (short_range + long_rows)


def solution(mesh):
    in_specs = (P("gx", "gy", None), P(None, "gx", "gy", None), P(), P(), P())
    out_specs = P(None, "gx", "gy", None)
    return jax.shard_map(
        per_device, mesh=mesh, in_specs=in_specs, out_specs=out_specs, check_vma=False
    )
```

```python
import functools
import math

import jax
import jax.numpy as jnp
import numpy as np
from jax import lax
from jax.experimental import pallas as pl
from jax.experimental.pallas import tpu as pltpu
from jax.sharding import PartitionSpec as P

FACTOR = 4
RADIUS = 16
LONG_COUPLING = 16.0
HIGHEST = lax.Precision.HIGHEST
MESH = pl.DeviceIdType.MESH
F32 = jnp.float32

T_P, T_Q, T_A, T_B, T_G, T_W, T_ROWS = 0, 8, 16, 32, 48, 72, 80
C_ZF, C_ZI, C_ZD, C_YF, C_YI, C_ROWS = 0, 32, 64, 96, 608, 1120


def z_basis():
    n = np.arange(32)
    basis = np.zeros((2, 16, 32))
    norm = np.full((2, 16), 2.0 / 32)
    for g in range(16):
        basis[0, g] = np.cos(2 * np.pi * g * n / 32)
        basis[1, g] = np.sin(2 * np.pi * g * n / 32)
    basis[1, 0] = np.cos(np.pi * n)
    norm[:, 0] = 1.0 / 32
    return basis.reshape(32, 32), norm.reshape(32)


def y_basis(count):
    half = count // 2
    wave = np.array([m if m <= half else m - half for m in range(count)])
    y = np.arange(count)
    angle = 2 * np.pi / count * (wave[:, None] * y[None, :] % count)
    is_cos = (np.arange(count) <= half)[:, None]
    basis = np.where(is_cos, np.cos(angle), np.sin(angle))
    norm = np.where((wave == 0) | (wave == half), 1.0, 2.0) / count
    return basis, norm, wave


def shared_constants():
    out = np.zeros((C_ROWS, 128))
    zb, zn = z_basis()
    out[C_ZF : C_ZF + 32] = np.repeat(zb, 4, axis=1) / 64.0
    zi = zb * zn[:, None] * LONG_COUPLING
    out[C_ZI : C_ZI + 32] = np.repeat(zi, 4, axis=1)
    zd = 0.5 * (np.roll(zi, -1, axis=1) - np.roll(zi, 1, axis=1))
    out[C_ZD : C_ZD + 32] = np.repeat(zd, 4, axis=1)
    yb, yn, _ = y_basis(192)
    for tile in range(2):
        for half in range(2):
            fwd = np.zeros((128, 128))
            inv = np.zeros((128, 128))
            fwd[:96, :96] = yb[96 * half : 96 * half + 96, 96 * tile : 96 * tile + 96].T
            for jj in range(8):
                for p in range(14):
                    y = (12 * (8 * tile + jj) - 1 + p) % 192
                    cols = slice(96 * half, 96 * half + 96)
                    inv[:96, 16 * jj + p] = yb[cols, y] * yn[cols]
            row = C_YF + (2 * tile + half) * 128
            out[row : row + 128] = fwd
            row = C_YI + (2 * half + tile) * 128
            out[row : row + 128] = inv
    return out.astype(np.float32)


def solve_tables(chips):
    n = 8 * chips
    out = np.zeros((17, 2, T_ROWS, 128))
    _, _, wave = y_basis(192)
    for kz in range(17):
        for half in range(2):
            t = out[kz, half]
            ky = wave[96 * half : 96 * half + 96]
            a = np.ones(128)
            a[:96] = (2 - 2 * np.cos(2 * np.pi * ky / 192)) + (2 - 2 * np.cos(2 * np.pi * kz / 32))
            zero = np.zeros(128, bool)
            zero[:96] = (ky == 0) & (kz == 0)
            a[zero] = 1.0
            r = 1 + a / 2 - np.sqrt(a + a * a / 4)
            den = (1 / r - r) * (1 - r**n)
            pick = lambda general, special: np.where(zero, special, general)
            for x8 in range(8):
                t[T_P + x8] = pick(r ** float(-x8), 1.0)
                t[T_Q + x8] = pick(r**x8, float(x8))
            for o in range(10):
                x8 = o - 1
                t[T_A + o] = pick(r ** float(x8) / den, -x8 / 2 + x8 * x8 / (2 * n))
                t[T_B + o] = pick(r ** float(-x8) / den, -x8 / n)
            for o in range(17):
                d = abs(o - 8)
                t[T_G + o] = pick((r**d + r ** (n - d)) / den, -d * (n - d) / (2 * n))
            t[T_W] = pick(r**8, 1.0)
    return out.astype(np.float32)


def dot(a, b):
    return lax.dot_general(a, b, (((1,), (0,)), ((), ())), precision=HIGHEST, preferred_element_type=F32)


def dot_nt(a, b):
    return lax.dot_general(a, b, (((1,), (1,)), ((), ())), precision=HIGHEST, preferred_element_type=F32)


def wrap(value, count):
    return lax.rem(value + count, count)


def send_order(chips):
    ring = min(16, chips)
    def hops(step):
        along = step % ring
        return min(along, ring - along) + (2 if step >= ring else 0)
    return sorted(range(1, chips), key=lambda step: (-hops(step), step))


def band_rows(taps, rows, shift):
    lane = lax.broadcasted_iota(jnp.int32, (1, 128), 1)
    row = jnp.zeros((1, 128), F32)
    for tap in range(2 * RADIUS + 1):
        row = jnp.where(lane == tap, taps[tap], row)
    return pltpu.roll(jnp.broadcast_to(row, (rows, 128)), shift % 128, 1, stride=1, stride_axis=0)


def convolve_rows(padded, mid, smooth, deriv, first):
    for group in range(0, 16, 8):
        sums = [[None] * 8, [None] * 8]
        for tap in range(2 * RADIUS + 1):
            weights = (smooth[tap], deriv[tap])
            for i in range(8):
                cells = padded[group + i + tap, pl.ds(first, 8), :]
                for f in range(2):
                    term = cells * weights[f]
                    sums[f][i] = term if tap == 0 else sums[f][i] + term
        for f in range(2):
            for i in range(8):
                mid[f, group + i, pl.ds(first, 8), :] = sums[f][i]


NEAR_LAST = (8, 7, 9, 6, 10, 5, 11, 4, 12, 3, 13, 2, 14, 1, 15)


def kernel(
    gx_count, smooth, deriv, kick, density, momenta, cst_hbm, tab_hbm, out,
    padded, mid, bands, cst, tab, m1, r1, fs, pair, mom, r2, os_, pair2, ps, r3,
    load_sem, strip_send, strip_recv, tile_send, tile_recv, corner_send, corner_recv,
    m_send, m_recv, p_send, p_recv,
):
    gx = lax.axis_index("gx")
    gy = lax.axis_index("gy")
    chips = gx_count // 2
    core = lax.rem(gx, 2)
    chip = gx // 2
    partner = gx + 1 - 2 * core
    outer = wrap(gx + 2 * core - 1, gx_count)

    barrier = pltpu.get_barrier_semaphore()

    def greet(device):
        pl.semaphore_signal(barrier, inc=1, device_id=device, device_id_type=MESH)

    for step in send_order(chips):
        greet({"gx": 2 * lax.rem(chip + step, chips) + core})
    for step in NEAR_LAST:
        greet({"gy": lax.rem(gy + step, 16)})
    greet({"gx": outer})
    greet({"gx": partner})

    is_zero = (gy == 0).astype(jnp.int32)
    loads = [
        pltpu.make_async_copy(density, padded.at[16:32, 16:64], load_sem.at[0]),
        pltpu.make_async_copy(cst_hbm, cst, load_sem.at[1]),
        pltpu.make_async_copy(tab_hbm.at[gy, core], tab.at[0], load_sem.at[2]),
        pltpu.make_async_copy(tab_hbm.at[gy + 16 * is_zero, core], tab.at[1], load_sem.at[3]),
    ]
    for load in loads:
        load.start()
    load_momenta = pltpu.make_async_copy(momenta, out, load_sem.at[4])
    load_momenta.start()
    bands[0:48] = band_rows(smooth, 48, 0)
    bands[48:96] = band_rows(deriv, 48, 0)
    bands[96:224] = band_rows(smooth, 128, -RADIUS)
    bands[224:352] = band_rows(deriv, 128, -RADIUS)
    for load in loads:
        load.wait()

    lane = lax.broadcasted_iota(jnp.int32, (48, 128), 1)
    block = lax.broadcasted_iota(jnp.int32, (48, 128), 0) // 4
    placed = (lane == block + 12 * lax.rem(gy, 8)).astype(F32)
    zf = cst[C_ZF : C_ZF + 32]
    for xl in range(4):
        rows = padded[16 + 4 * xl, 16:64]
        for fine in range(1, 4):
            rows = rows + padded[16 + 4 * xl + fine, 16:64]
        spread = dot(dot_nt(zf, rows), placed)
        for c in range(2):
            m1[:, c * 4 + xl, :] = spread[16 * c : 16 * c + 16]

    pl.semaphore_wait(barrier, (chips - 1) + 15 + 2)

    def remote(src, dst, send_sem, recv_sem, device):
        return pltpu.make_async_remote_copy(
            src_ref=src, dst_ref=dst, send_sem=send_sem, recv_sem=recv_sem,
            device_id=device, device_id_type=MESH,
        )

    for step in NEAR_LAST:
        target = lax.rem(gy + step, 16)
        remote(m1.at[target], r1.at[gy], m_send.at[0], m_recv.at[0], {"gy": target}).start()
    below, above = wrap(gy - 1, 16), lax.rem(gy + 1, 16)
    strips = [
        remote(padded.at[16:32, 16:32], padded.at[16:32, 64:80], strip_send.at[0], strip_recv.at[0], {"gy": below}),
        remote(padded.at[16:32, 48:64], padded.at[16:32, 0:16], strip_send.at[1], strip_recv.at[1], {"gy": above}),
    ]
    back, ahead = wrap(gx - 1, gx_count), lax.rem(gx + 1, gx_count)
    tiles = [
        remote(padded.at[16:32, 16:64], padded.at[32:48, 16:64], tile_send.at[0], tile_recv.at[0], {"gx": back}),
        remote(padded.at[16:32, 16:64], padded.at[0:16, 16:64], tile_send.at[1], tile_recv.at[1], {"gx": ahead}),
    ]
    for copy in strips + tiles:
        copy.start()

    r1[gy] = m1[gy]
    pltpu.make_async_copy(r1.at[0:15], r1.at[0:15], m_recv.at[0]).wait()
    low = r1[0]
    high = r1[8]
    for j in range(1, 8):
        low = low + r1[j]
        high = high + r1[8 + j]
    for half in range(2):
        first = C_YF + half * 128
        second = C_YF + (2 + half) * 128
        fs[half] = dot(low, cst[first : first + 128]) + dot(high, cst[second : second + 128])
    swap = remote(fs.at[1 - core], pair.at[core], p_send.at[0], p_recv.at[0], {"gx": partner})
    swap.start()
    pair[core] = fs[core]
    swap.wait_recv()

    e0 = pair[0]
    e1 = pair[1]
    for pq, table in ((0, T_P), (1, T_Q)):
        for c in range(2):
            rows = slice(4 * c, 4 * c + 4)
            terms = e0[rows] * tab[c, table : table + 4] + e1[rows] * tab[c, table + 4 : table + 8]
            mom[2 * pq + c : 2 * pq + c + 1, :] = jnp.sum(terms, axis=0, keepdims=True)
    for step in send_order(chips):
        target = 2 * lax.rem(chip + step, chips) + core
        remote(mom, r2.at[step], m_send.at[1], m_recv.at[1], {"gx": target}).start()

    for copy in strips:
        copy.wait_recv()
    corners = []
    for side, cols in enumerate((slice(0, 16), slice(64, 80))):
        corners.append(remote(padded.at[16:32, cols], padded.at[32:48, cols], corner_send.at[2 * side], corner_recv.at[2 * side], {"gx": back}))
        corners.append(remote(padded.at[16:32, cols], padded.at[0:16, cols], corner_send.at[2 * side + 1], corner_recv.at[2 * side + 1], {"gx": ahead}))
    for copy in corners:
        copy.start()
    for copy in tiles:
        copy.wait_recv()

    @pl.loop(2, 8)
    def _(k):
        convolve_rows(padded, mid, smooth, deriv, pl.multiple_of(8 * k, 8))

    pltpu.make_async_copy(r2.at[1:chips], r2.at[1:chips], m_recv.at[1]).wait()
    ratio = jnp.concatenate([tab[c, T_W : T_W + 1] for c in (0, 1, 0, 1)], axis=0)
    is_first = lax.broadcasted_iota(jnp.int32, (4, 128), 0) < 2
    total = jnp.zeros((4, 128), F32)
    ramp = jnp.zeros((4, 128), F32)
    for step in range(chips - 1, 0, -1):
        total = (total + jnp.where(is_first, r2[step], r2[chips - step])) * ratio
        ramp = ramp + total
    is_mean = (gy == 0) & (core == 0)
    row8 = lax.broadcasted_iota(jnp.int32, (8, 128), 0)
    lane8 = lax.broadcasted_iota(jnp.int32, (8, 128), 1)
    for ct in range(2):
        for c in range(2):
            o = 4 * ct
            phi = (
                tab[c, T_A + o : T_A + o + 8] * total[c : c + 1]
                + tab[c, T_B + o : T_B + o + 8] * total[2 + c : 3 + c]
            )
            if c == 0:
                weight = jnp.where((lane8 == 0) & is_mean, (row8 + (o - 1)).astype(F32) * (1.0 / chips), 0.0)
                phi = phi + weight * ramp[0:1]
            for x8 in range(8):
                source = (e0 if x8 < 4 else e1)[c * 4 + x8 % 4 : c * 4 + x8 % 4 + 1]
                start = T_G + 7 + o - x8
                phi = phi + tab[c, start : start + 8] * source
            os_[ct, c * 8 : c * 8 + 8, :] = phi
    swap2 = remote(os_.at[1 - core], pair2.at[core], p_send.at[1], p_recv.at[1], {"gx": partner})
    swap2.start()
    pair2[core] = os_[core]
    swap2.wait_recv()

    h0 = pair2[0]
    h1 = pair2[1]
    for tile in range(2):
        first = C_YI + tile * 128
        second = C_YI + (2 + tile) * 128
        phi = dot(h0, cst[first : first + 128]) + dot(h1, cst[second : second + 128])
        for odd in range(2):
            parts = [phi[0:8], phi[8:16]]
            parts[1 - odd] = pltpu.roll(parts[1 - odd], 64, 1)
            ps[2 * tile + odd] = jnp.where(lane8 < 64, parts[0], parts[1])
    for step in NEAR_LAST:
        target = lax.rem(gy + step, 16)
        remote(ps.at[target // 4], r3.at[gy], m_send.at[2], m_recv.at[2], {"gy": target}).start()
    r3[gy] = ps[gy // 4]

    for copy in corners:
        copy.wait_recv()

    @pl.loop(0, 4)
    def _(k):
        convolve_rows(padded, mid, smooth, deriv, pl.multiple_of(8 * (k + 6 * (k // 2)), 8))

    load_momenta.wait()
    time_step = kick[0]

    @pl.loop(0, 4)
    def _(k):
        cols = bands[0:96, 0:80]
        firsts, seconds, thirds = [], [], []
        for u in range(4):
            x = 4 * k + u
            firsts.append(dot(cols[0:48], mid[1, x]))
            both = dot(cols, mid[0, x])
            thirds.append(both[0:48])
            seconds.append(both[48:96])
        smoothed = dot_nt(jnp.concatenate(firsts + seconds, axis=0), bands[96:224])
        derived = dot_nt(jnp.concatenate(thirds, axis=0), bands[224:352])
        for u in range(4):
            x = 4 * k + u
            out[0, x] = out[0, x] + time_step * smoothed[48 * u : 48 * u + 48]
            out[1, x] = out[1, x] + time_step * smoothed[48 * (4 + u) : 48 * (4 + u) + 48]
            out[2, x] = out[2, x] + time_step * derived[48 * u : 48 * u + 48]

    here = block + 16 * lax.rem(gy, 4) + 1
    at_cell = (lane == here).astype(F32)
    slope = 0.5 * (lane == here + 1).astype(F32) - 0.5 * (lane == here - 1).astype(F32)
    zi = cst[C_ZI : C_ZI + 32] * time_step
    zd = cst[C_ZD : C_ZD + 32] * time_step
    pltpu.make_async_copy(r3.at[0:15], r3.at[0:15], m_recv.at[2]).wait()
    along = []
    across = []
    for i in range(6):
        tile = r3[:, i, :]
        coeffs = jnp.concatenate([tile, pltpu.roll(tile, 64, 1)], axis=0)
        along.append(dot_nt(at_cell, coeffs))
        if 1 <= i <= 4:
            across.append(dot_nt(slope, coeffs))
    for xl in range(4):
        for d, force in enumerate((
            dot(0.5 * (along[xl + 2] - along[xl]), zi),
            dot(across[xl], zi),
            dot(along[xl + 1], zd),
        )):
            for fine in range(4):
                out[d, 4 * xl + fine] = out[d, 4 * xl + fine] + force

    for copy in strips + tiles + corners + [swap, swap2]:
        copy.wait_send()
    pltpu.make_async_copy(m1.at[0:15], m1.at[0:15], m_send.at[0]).wait()
    pltpu.make_async_copy(r2.at[1:chips], r2.at[1:chips], m_send.at[1]).wait()
    pltpu.make_async_copy(r3.at[0:15], r3.at[0:15], m_send.at[2]).wait()


def per_device(density, momenta, smooth_taps, deriv_taps, kick_step):
    gx_count = lax.axis_size("gx")
    chips = gx_count // 2
    any_spec = pl.BlockSpec(memory_space=pl.ANY)
    vmem_spec = pl.BlockSpec(memory_space=pltpu.VMEM)
    smem_spec = pl.BlockSpec(memory_space=pltpu.SMEM)
    vm = lambda *shape: pltpu.VMEM(shape, F32)
    dma = lambda n: pltpu.SemaphoreType.DMA((n,))
    return pl.pallas_call(
        functools.partial(kernel, gx_count),
        out_shape=pltpu.VMEM((3, 16, 48, 128), F32),
        in_specs=[smem_spec] * 3 + [any_spec] * 4,
        out_specs=vmem_spec,
        scratch_shapes=[
            vm(48, 80, 128), vm(2, 16, 80, 128), vm(352, 128),
            vm(C_ROWS, 128), vm(2, T_ROWS, 128), vm(16, 8, 128), vm(16, 8, 128), vm(2, 8, 128), vm(2, 8, 128),
            vm(4, 128), vm(chips, 4, 128), vm(2, 16, 128), vm(2, 16, 128), vm(4, 8, 128), vm(16, 8, 128),
            dma(5), dma(2), dma(2), dma(2), dma(2), dma(4), dma(4), dma(3), dma(3), dma(2), dma(2),
        ],
        compiler_params=pltpu.CompilerParams(collective_id=0, has_side_effects=True),
    )(
        smooth_taps, deriv_taps, kick_step.reshape(1), density, momenta,
        jnp.asarray(shared_constants()), jnp.asarray(solve_tables(chips)),
    )


def solution(mesh):
    in_specs = (P("gx", "gy", None), P(None, "gx", "gy", None), P(), P(), P())
    out_specs = P(None, "gx", "gy", None)
    return jax.shard_map(
        per_device, mesh=mesh, in_specs=in_specs, out_specs=out_specs, check_vma=False
    )
```

```python
import functools
import math

import jax
import jax.numpy as jnp
import numpy as np
from jax import lax
from jax.experimental import pallas as pl
from jax.experimental.pallas import tpu as pltpu
from jax.sharding import PartitionSpec as P

FACTOR = 4
RADIUS = 16
LONG_COUPLING = 16.0
HIGHEST = lax.Precision.HIGHEST
MESH = pl.DeviceIdType.MESH
F32 = jnp.float32

T_P, T_Q, T_A, T_B, T_G, T_W, T_ROWS = 0, 8, 16, 32, 48, 72, 80
C_ZF, C_ZI, C_ZD, C_YF, C_YI, C_ROWS = 0, 32, 64, 96, 608, 1120


def z_basis():
    n = np.arange(32)
    basis = np.zeros((2, 16, 32))
    norm = np.full((2, 16), 2.0 / 32)
    for g in range(16):
        basis[0, g] = np.cos(2 * np.pi * g * n / 32)
        basis[1, g] = np.sin(2 * np.pi * g * n / 32)
    basis[1, 0] = np.cos(np.pi * n)
    norm[:, 0] = 1.0 / 32
    return basis.reshape(32, 32), norm.reshape(32)


def y_basis(count):
    half = count // 2
    wave = np.array([m if m <= half else m - half for m in range(count)])
    y = np.arange(count)
    angle = 2 * np.pi / count * (wave[:, None] * y[None, :] % count)
    is_cos = (np.arange(count) <= half)[:, None]
    basis = np.where(is_cos, np.cos(angle), np.sin(angle))
    norm = np.where((wave == 0) | (wave == half), 1.0, 2.0) / count
    return basis, norm, wave


def shared_constants():
    out = np.zeros((C_ROWS, 128))
    zb, zn = z_basis()
    out[C_ZF : C_ZF + 32] = np.repeat(zb, 4, axis=1) / 64.0
    zi = zb * zn[:, None] * LONG_COUPLING
    out[C_ZI : C_ZI + 32] = np.repeat(zi, 4, axis=1)
    zd = 0.5 * (np.roll(zi, -1, axis=1) - np.roll(zi, 1, axis=1))
    out[C_ZD : C_ZD + 32] = np.repeat(zd, 4, axis=1)
    yb, yn, _ = y_basis(192)
    for tile in range(2):
        for half in range(2):
            fwd = np.zeros((128, 128))
            inv = np.zeros((128, 128))
            fwd[:96, :96] = yb[96 * half : 96 * half + 96, 96 * tile : 96 * tile + 96].T
            for jj in range(8):
                for p in range(14):
                    y = (12 * (8 * tile + jj) - 1 + p) % 192
                    cols = slice(96 * half, 96 * half + 96)
                    inv[:96, 16 * jj + p] = yb[cols, y] * yn[cols]
            row = C_YF + (2 * tile + half) * 128
            out[row : row + 128] = fwd
            row = C_YI + (2 * half + tile) * 128
            out[row : row + 128] = inv
    return out.astype(np.float32)


def solve_tables(chips):
    n = 8 * chips
    out = np.zeros((17, 2, T_ROWS, 128))
    _, _, wave = y_basis(192)
    for kz in range(17):
        for half in range(2):
            t = out[kz, half]
            ky = wave[96 * half : 96 * half + 96]
            a = np.ones(128)
            a[:96] = (2 - 2 * np.cos(2 * np.pi * ky / 192)) + (2 - 2 * np.cos(2 * np.pi * kz / 32))
            zero = np.zeros(128, bool)
            zero[:96] = (ky == 0) & (kz == 0)
            a[zero] = 1.0
            r = 1 + a / 2 - np.sqrt(a + a * a / 4)
            den = (1 / r - r) * (1 - r**n)
            pick = lambda general, special: np.where(zero, special, general)
            for x8 in range(8):
                t[T_P + x8] = pick(r ** float(-x8), 1.0)
                t[T_Q + x8] = pick(r**x8, float(x8))
            for o in range(10):
                x8 = o - 1
                t[T_A + o] = pick(r ** float(x8) / den, -x8 / 2 + x8 * x8 / (2 * n))
                t[T_B + o] = pick(r ** float(-x8) / den, -x8 / n)
            for o in range(17):
                d = abs(o - 8)
                t[T_G + o] = pick((r**d + r ** (n - d)) / den, -d * (n - d) / (2 * n))
            t[T_W] = pick(r**8, 1.0)
    return out.astype(np.float32)


def dot(a, b):
    return lax.dot_general(a, b, (((1,), (0,)), ((), ())), precision=HIGHEST, preferred_element_type=F32)


def dot_nt(a, b):
    return lax.dot_general(a, b, (((1,), (1,)), ((), ())), precision=HIGHEST, preferred_element_type=F32)


def wrap(value, count):
    return lax.rem(value + count, count)


def send_order(chips):
    ring = min(16, chips)
    def hops(step):
        along = step % ring
        return min(along, ring - along) + (2 if step >= ring else 0)
    return sorted(range(1, chips), key=lambda step: (-hops(step), step))


def band_rows(taps, rows, shift):
    lane = lax.broadcasted_iota(jnp.int32, (1, 128), 1)
    row = jnp.zeros((1, 128), F32)
    for tap in range(2 * RADIUS + 1):
        row = jnp.where(lane == tap, taps[tap], row)
    return pltpu.roll(jnp.broadcast_to(row, (rows, 128)), shift % 128, 1, stride=1, stride_axis=0)


def convolve_rows(padded, mid, smooth, deriv, first):
    for group in range(0, 16, 8):
        sums = [[None] * 8, [None] * 8]
        for tap in range(2 * RADIUS + 1):
            weights = (smooth[tap], deriv[tap])
            for i in range(8):
                cells = padded[group + i + tap, pl.ds(first, 8), :]
                for f in range(2):
                    term = cells * weights[f]
                    sums[f][i] = term if tap == 0 else sums[f][i] + term
        for f in range(2):
            for i in range(8):
                mid[f, group + i, pl.ds(first, 8), :] = sums[f][i]


NEAR_LAST = (8, 7, 9, 6, 10, 5, 11, 4, 12, 3, 13, 2, 14, 1, 15)


def kernel(
    gx_count, smooth, deriv, kick, density, momenta, cst_hbm, tab_hbm, out,
    padded, mid, bands, cst, tab, m1, r1, fs, pair, mom, r2, os_, pair2, ps, r3,
    load_sem, strip_send, strip_recv, tile_send, tile_recv, corner_send, corner_recv,
    m_send, m_recv, p_send, p_recv,
):
    gx = lax.axis_index("gx")
    gy = lax.axis_index("gy")
    chips = gx_count // 2
    core = lax.rem(gx, 2)
    chip = gx // 2
    partner = gx + 1 - 2 * core
    outer = wrap(gx + 2 * core - 1, gx_count)

    barrier = pltpu.get_barrier_semaphore()

    def greet(device):
        pl.semaphore_signal(barrier, inc=1, device_id=device, device_id_type=MESH)

    for step in send_order(chips):
        greet({"gx": 2 * lax.rem(chip + step, chips) + core})
    for step in NEAR_LAST:
        greet({"gy": lax.rem(gy + step, 16)})
    greet({"gx": outer})
    greet({"gx": partner})

    is_zero = (gy == 0).astype(jnp.int32)
    loads = [
        pltpu.make_async_copy(density, padded.at[16:32, 16:64], load_sem.at[0]),
        pltpu.make_async_copy(cst_hbm, cst, load_sem.at[1]),
        pltpu.make_async_copy(tab_hbm.at[gy, core], tab.at[0], load_sem.at[2]),
        pltpu.make_async_copy(tab_hbm.at[gy + 16 * is_zero, core], tab.at[1], load_sem.at[3]),
    ]
    for load in loads:
        load.start()
    load_momenta = pltpu.make_async_copy(momenta, out, load_sem.at[4])
    load_momenta.start()
    bands[0:48] = band_rows(smooth, 48, 0)
    bands[48:96] = band_rows(deriv, 48, 0)
    bands[96:224] = band_rows(smooth, 128, -RADIUS)
    bands[224:352] = band_rows(deriv, 128, -RADIUS)
    for load in loads:
        load.wait()

    lane = lax.broadcasted_iota(jnp.int32, (48, 128), 1)
    block = lax.broadcasted_iota(jnp.int32, (48, 128), 0) // 4
    placed = (lane == block + 12 * lax.rem(gy, 8)).astype(F32)
    zf = cst[C_ZF : C_ZF + 32]
    for xl in range(4):
        rows = padded[16 + 4 * xl, 16:64]
        for fine in range(1, 4):
            rows = rows + padded[16 + 4 * xl + fine, 16:64]
        spread = dot(dot_nt(zf, rows), placed)
        for c in range(2):
            m1[:, c * 4 + xl, :] = spread[16 * c : 16 * c + 16]

    pl.semaphore_wait(barrier, (chips - 1) + 15 + 2)

    def remote(src, dst, send_sem, recv_sem, device):
        return pltpu.make_async_remote_copy(
            src_ref=src, dst_ref=dst, send_sem=send_sem, recv_sem=recv_sem,
            device_id=device, device_id_type=MESH,
        )

    for step in NEAR_LAST:
        target = lax.rem(gy + step, 16)
        remote(m1.at[target], r1.at[gy], m_send.at[0], m_recv.at[0], {"gy": target}).start()
    below, above = wrap(gy - 1, 16), lax.rem(gy + 1, 16)
    strips = [
        remote(padded.at[16:32, 16:32], padded.at[16:32, 64:80], strip_send.at[0], strip_recv.at[0], {"gy": below}),
        remote(padded.at[16:32, 48:64], padded.at[16:32, 0:16], strip_send.at[1], strip_recv.at[1], {"gy": above}),
    ]
    back, ahead = wrap(gx - 1, gx_count), lax.rem(gx + 1, gx_count)
    tiles = [
        remote(padded.at[16:32, 16:64], padded.at[32:48, 16:64], tile_send.at[0], tile_recv.at[0], {"gx": back}),
        remote(padded.at[16:32, 16:64], padded.at[0:16, 16:64], tile_send.at[1], tile_recv.at[1], {"gx": ahead}),
    ]
    for copy in strips + tiles:
        copy.start()

    r1[gy] = m1[gy]
    pltpu.make_async_copy(r1.at[0:15], r1.at[0:15], m_recv.at[0]).wait()
    low = r1[0]
    high = r1[8]
    for j in range(1, 8):
        low = low + r1[j]
        high = high + r1[8 + j]
    for half in range(2):
        first = C_YF + half * 128
        second = C_YF + (2 + half) * 128
        fs[half] = dot(low, cst[first : first + 128]) + dot(high, cst[second : second + 128])
    swap = remote(fs.at[1 - core], pair.at[core], p_send.at[0], p_recv.at[0], {"gx": partner})
    swap.start()
    pair[core] = fs[core]
    swap.wait_recv()

    e0 = pair[0]
    e1 = pair[1]
    for pq, table in ((0, T_P), (1, T_Q)):
        for c in range(2):
            rows = slice(4 * c, 4 * c + 4)
            terms = e0[rows] * tab[c, table : table + 4] + e1[rows] * tab[c, table + 4 : table + 8]
            mom[2 * pq + c : 2 * pq + c + 1, :] = jnp.sum(terms, axis=0, keepdims=True)
    for step in send_order(chips):
        target = 2 * lax.rem(chip + step, chips) + core
        remote(mom, r2.at[step], m_send.at[1], m_recv.at[1], {"gx": target}).start()

    for copy in strips:
        copy.wait_recv()
    corners = []
    for side, cols in enumerate((slice(0, 16), slice(64, 80))):
        corners.append(remote(padded.at[16:32, cols], padded.at[32:48, cols], corner_send.at[2 * side], corner_recv.at[2 * side], {"gx": back}))
        corners.append(remote(padded.at[16:32, cols], padded.at[0:16, cols], corner_send.at[2 * side + 1], corner_recv.at[2 * side + 1], {"gx": ahead}))
    for copy in corners:
        copy.start()
    for copy in tiles:
        copy.wait_recv()

    @pl.loop(2, 8)
    def _(k):
        convolve_rows(padded, mid, smooth, deriv, pl.multiple_of(8 * k, 8))

    pltpu.make_async_copy(r2.at[1:chips], r2.at[1:chips], m_recv.at[1]).wait()
    ratio = jnp.concatenate([tab[c, T_W : T_W + 1] for c in (0, 1, 0, 1)], axis=0)
    is_first = lax.broadcasted_iota(jnp.int32, (4, 128), 0) < 2
    is_mean = (gy == 0) & (core == 0)
    lane1 = lax.broadcasted_iota(jnp.int32, (1, 128), 1)
    level = jnp.where((lane1 == 0) & is_mean, mom[0:1, :] * 0.125, 0.0)
    none = jnp.zeros((1, 128), F32)
    uniform = jnp.concatenate([8.0 * level, none, 28.0 * level, none], axis=0)
    total = jnp.zeros((4, 128), F32)
    ramp = jnp.zeros((4, 128), F32)
    for step in range(chips - 1, 0, -1):
        total = (total + (jnp.where(is_first, r2[step], r2[chips - step]) - uniform)) * ratio
        ramp = ramp + total
    row8 = lax.broadcasted_iota(jnp.int32, (8, 128), 0)
    lane8 = lax.broadcasted_iota(jnp.int32, (8, 128), 1)
    for ct in range(2):
        for c in range(2):
            o = 4 * ct
            phi = (
                tab[c, T_A + o : T_A + o + 8] * total[c : c + 1]
                + tab[c, T_B + o : T_B + o + 8] * total[2 + c : 3 + c]
            )
            if c == 0:
                weight = jnp.where((lane8 == 0) & is_mean, (row8 + (o - 1)).astype(F32) * (1.0 / chips), 0.0)
                phi = phi + weight * ramp[0:1]
            for x8 in range(8):
                source = (e0 if x8 < 4 else e1)[c * 4 + x8 % 4 : c * 4 + x8 % 4 + 1]
                if c == 0:
                    source = source - level
                start = T_G + 7 + o - x8
                phi = phi + tab[c, start : start + 8] * source
            os_[ct, c * 8 : c * 8 + 8, :] = phi
    swap2 = remote(os_.at[1 - core], pair2.at[core], p_send.at[1], p_recv.at[1], {"gx": partner})
    swap2.start()
    pair2[core] = os_[core]
    swap2.wait_recv()

    h0 = pair2[0]
    h1 = pair2[1]
    for tile in range(2):
        first = C_YI + tile * 128
        second = C_YI + (2 + tile) * 128
        phi = dot(h0, cst[first : first + 128]) + dot(h1, cst[second : second + 128])
        for odd in range(2):
            parts = [phi[0:8], phi[8:16]]
            parts[1 - odd] = pltpu.roll(parts[1 - odd], 64, 1)
            ps[2 * tile + odd] = jnp.where(lane8 < 64, parts[0], parts[1])
    for step in NEAR_LAST:
        target = lax.rem(gy + step, 16)
        remote(ps.at[target // 4], r3.at[gy], m_send.at[2], m_recv.at[2], {"gy": target}).start()
    r3[gy] = ps[gy // 4]

    for copy in corners:
        copy.wait_recv()

    @pl.loop(0, 4)
    def _(k):
        convolve_rows(padded, mid, smooth, deriv, pl.multiple_of(8 * (k + 6 * (k // 2)), 8))

    load_momenta.wait()
    time_step = kick[0]

    @pl.loop(0, 4)
    def _(k):
        cols = bands[0:96, 0:80]
        firsts, seconds, thirds = [], [], []
        for u in range(4):
            x = 4 * k + u
            firsts.append(dot(cols[0:48], mid[1, x]))
            both = dot(cols, mid[0, x])
            thirds.append(both[0:48])
            seconds.append(both[48:96])
        smoothed = dot_nt(jnp.concatenate(firsts + seconds, axis=0), bands[96:224])
        derived = dot_nt(jnp.concatenate(thirds, axis=0), bands[224:352])
        for u in range(4):
            x = 4 * k + u
            out[0, x] = out[0, x] + time_step * smoothed[48 * u : 48 * u + 48]
            out[1, x] = out[1, x] + time_step * smoothed[48 * (4 + u) : 48 * (4 + u) + 48]
            out[2, x] = out[2, x] + time_step * derived[48 * u : 48 * u + 48]

    here = block + 16 * lax.rem(gy, 4) + 1
    at_cell = (lane == here).astype(F32)
    slope = 0.5 * (lane == here + 1).astype(F32) - 0.5 * (lane == here - 1).astype(F32)
    zi = cst[C_ZI : C_ZI + 32] * time_step
    zd = cst[C_ZD : C_ZD + 32] * time_step
    pltpu.make_async_copy(r3.at[0:15], r3.at[0:15], m_recv.at[2]).wait()
    along = []
    across = []
    for i in range(6):
        tile = r3[:, i, :]
        coeffs = jnp.concatenate([tile, pltpu.roll(tile, 64, 1)], axis=0)
        along.append(dot_nt(at_cell, coeffs))
        if 1 <= i <= 4:
            across.append(dot_nt(slope, coeffs))
    for xl in range(4):
        for d, force in enumerate((
            dot(0.5 * (along[xl + 2] - along[xl]), zi),
            dot(across[xl], zi),
            dot(along[xl + 1], zd),
        )):
            for fine in range(4):
                out[d, 4 * xl + fine] = out[d, 4 * xl + fine] + force

    for copy in strips + tiles + corners + [swap, swap2]:
        copy.wait_send()
    pltpu.make_async_copy(m1.at[0:15], m1.at[0:15], m_send.at[0]).wait()
    pltpu.make_async_copy(r2.at[1:chips], r2.at[1:chips], m_send.at[1]).wait()
    pltpu.make_async_copy(r3.at[0:15], r3.at[0:15], m_send.at[2]).wait()


def per_device(density, momenta, smooth_taps, deriv_taps, kick_step):
    gx_count = lax.axis_size("gx")
    chips = gx_count // 2
    any_spec = pl.BlockSpec(memory_space=pl.ANY)
    vmem_spec = pl.BlockSpec(memory_space=pltpu.VMEM)
    smem_spec = pl.BlockSpec(memory_space=pltpu.SMEM)
    vm = lambda *shape: pltpu.VMEM(shape, F32)
    dma = lambda n: pltpu.SemaphoreType.DMA((n,))
    return pl.pallas_call(
        functools.partial(kernel, gx_count),
        out_shape=pltpu.VMEM((3, 16, 48, 128), F32),
        in_specs=[smem_spec] * 3 + [any_spec] * 4,
        out_specs=vmem_spec,
        scratch_shapes=[
            vm(48, 80, 128), vm(2, 16, 80, 128), vm(352, 128),
            vm(C_ROWS, 128), vm(2, T_ROWS, 128), vm(16, 8, 128), vm(16, 8, 128), vm(2, 8, 128), vm(2, 8, 128),
            vm(4, 128), vm(chips, 4, 128), vm(2, 16, 128), vm(2, 16, 128), vm(4, 8, 128), vm(16, 8, 128),
            dma(5), dma(2), dma(2), dma(2), dma(2), dma(4), dma(4), dma(3), dma(3), dma(2), dma(2),
        ],
        compiler_params=pltpu.CompilerParams(collective_id=0, has_side_effects=True),
    )(
        smooth_taps, deriv_taps, kick_step.reshape(1), density, momenta,
        jnp.asarray(shared_constants()), jnp.asarray(solve_tables(chips)),
    )


def solution(mesh):
    in_specs = (P("gx", "gy", None), P(None, "gx", "gy", None), P(), P(), P())
    out_specs = P(None, "gx", "gy", None)
    return jax.shard_map(
        per_device, mesh=mesh, in_specs=in_specs, out_specs=out_specs, check_vma=False
    )
```
